64 devices in a mesh: mol: 4 (over x, y), occ: 16 (over z, core).
Axes of the slice: x: 2, y: 2, z: 8, core: 2. Of those that a mesh axis runs over, the one named last changes fastest.
The devices are a block of a 4x4x8 slice.
Arguments:
- b_ints: bfloat16 [64, 672, 32, 160], P('mol', None, 'occ'), parts along dimension 0
- eps_occ: float32 [64, 32], P('mol'), parts along dimension 0
- eps_vir: float32 [64, 160], P('mol'), parts along dimension 0
- active: int32 [64, 32], P('mol'), parts along dimension 0
Outputs:
- output 1: float32 [64, 32], P('mol', 'occ'), parts along dimension 0
- output 2: float32 [64], P('mol'), parts along dimension 0
There are 4 independent parts. The reference program is written for one: setup_inputs(seed, part) draws one part's arguments, and reference() takes and returns one part's arrays. A program takes and returns all parts, laid end to end along the dimension named above; each array names one.
All inputs are finite; a program needn't handle non-finite values.
Results may differ from the reference program's by a relative error of at most 0.001.
Values are sent between devices in bfloat16 or wider.
A program may use at most 768 MiB of HBM per device.

```python
import jax
import jax.numpy as jnp
from jax import lax

FRAMES = 16
N_OCC = 32
N_VIR = 160
N_AUX = 672

B_SCALE = (N_OCC * N_VIR * N_VIR * N_AUX) ** -0.25


def setup_inputs(seed: int = 0, part: int = 0) -> dict:
    key_part = jax.random.fold_in(jax.random.key(seed), part)
    k_ints, k_scale, k_occ, k_vir, k_act = jax.random.split(key_part, 5)
    row_scale = jnp.exp(0.35 * jax.random.normal(k_scale, (FRAMES, 1, N_OCC, 1), jnp.float32) - 0.1225)
    b_ints = (jax.random.normal(k_ints, (FRAMES, N_AUX, N_OCC, N_VIR), jnp.float32) * row_scale * B_SCALE).astype(jnp.bfloat16)
    eps_occ = -1.6 + 1.3 * jnp.sort(jax.random.uniform(k_occ, (FRAMES, N_OCC), jnp.float32), axis=1)
    eps_vir = 0.2 + 2.8 * jnp.sort(jax.random.uniform(k_vir, (FRAMES, N_VIR), jnp.float32), axis=1)
    n_frozen = jax.random.randint(k_act, (FRAMES, 1), 1, N_OCC // 4 + 1)
    active = (jnp.arange(N_OCC)[None, :] >= n_frozen).astype(jnp.int32)
    return {"b_ints": b_ints, "eps_occ": eps_occ, "eps_vir": eps_vir, "active": active}


def reference(b_ints, eps_occ, eps_vir, active):
    def frame_pairs(frame_args):
        b_frame, occ_e, vir_e, act_f = frame_args
        act_w = act_f.astype(jnp.float32)
        b_flat = b_frame.reshape(N_AUX, N_OCC * N_VIR)
        vir_sum = vir_e[:, None, None] + vir_e[None, None, :]

        def row_energy(row_idx):
            b_row = b_frame[:, row_idx, :]
            k_pair = jnp.dot(b_row.T, b_flat, preferred_element_type=jnp.float32).reshape(N_VIR, N_OCC, N_VIR)
            denominator = occ_e[row_idx] + occ_e[None, :, None] - vir_sum
            pair_terms = k_pair * (2.0 * k_pair - jnp.transpose(k_pair, (2, 1, 0))) / denominator
            return act_w[row_idx] * jnp.sum(jnp.sum(pair_terms, axis=(0, 2)) * act_w)

        e_row = lax.map(row_energy, jnp.arange(N_OCC))
        return e_row, jnp.sum(e_row)

    e_pair, energy = lax.map(frame_pairs, (b_ints, eps_occ, eps_vir, active))
    return e_pair, energy
```

```python
import functools

import jax
import jax.numpy as jnp
from jax import lax
from jax.experimental import pallas as pl
from jax.experimental.pallas import tpu as pltpu
from jax.sharding import PartitionSpec as P

MESH = pl.DeviceIdType.MESH
CORES = 2
LANES = 128


def offsets(n_chip):
    half = n_chip // 2
    order = [(0, 0), (0, 1)]
    for dist in range(half - 1, 0, -1):
        for core in range(CORES):
            order += [(dist, core), (-dist, core)]
    relayed = [(half, core) for core in range(CORES)]
    return order + relayed


def kernel(n_dev, b_hbm, eps_ref, act_ref, vir_ref, out_ref, local, blocks, rest_out, rest_in, relay, relay_rest, vir_sum, acc, result, eps_slot, act_slot, load_sem, own_sem, send_sem, recv_sem, rest_send_sem, rest_recv_sem, hop_send_sem, hop_recv_sem, hop_rest_send_sem, hop_rest_recv_sem, res_send_sem, res_recv_sem):
    n_chip = n_dev // CORES
    half = n_chip // 2
    order = offsets(n_chip)
    n_loc, n_vir, n_aux = blocks.shape[1:]
    n_main = n_aux // LANES * LANES
    n_rest = n_aux - n_main
    fold = LANES // n_rest
    fold_rows = n_loc * n_vir // fold
    me = lax.axis_index("occ")
    chip, core = me // CORES, me % CORES

    def device(d_chip, d_core):
        return (chip + d_chip + n_chip) % n_chip * CORES + (core + d_core) % CORES

    load = pltpu.make_async_copy(b_hbm, local, load_sem)
    load.start()
    own = pltpu.make_async_copy(b_hbm.at[me], blocks.at[0], own_sem)
    own.start()
    barrier = pltpu.get_barrier_semaphore()
    for step in range(1, n_dev):
        pl.semaphore_signal(barrier, inc=1, device_id={"occ": (me + step) % n_dev}, device_id_type=MESH)

    for slot, (d_chip, d_core) in enumerate(order):
        owner = device(-d_chip, d_core)
        for orb in range(n_loc):
            eps_slot[slot, orb] = eps_ref[me, owner * n_loc + orb]
            act_slot[slot, orb] = act_ref[me, owner * n_loc + orb].astype(jnp.float32)
    vir_row = jnp.broadcast_to(vir_ref[pl.ds(me, 1), :], (n_vir, n_vir))
    vir_sum[...] = vir_row + vir_row.T
    acc[...] = jnp.zeros_like(acc)
    result[...] = jnp.zeros_like(result)
    load.wait()

    def pack(frame, carry):
        tail = local[frame, :, :, n_main:].reshape(n_loc * n_vir, n_rest)
        rest_out[frame] = jnp.concatenate([tail[part * fold_rows:(part + 1) * fold_rows] for part in range(fold)], axis=1)
        return carry

    lax.fori_loop(0, n_dev, pack, 0)
    pl.semaphore_wait(barrier, n_dev - 1)

    def main_copy(slot, target, frame):
        return pltpu.make_async_remote_copy(local.at[frame, :, :, pl.ds(0, n_main)], blocks.at[slot, :, :, pl.ds(0, n_main)], send_sem.at[slot], recv_sem.at[slot], device_id={"occ": target}, device_id_type=MESH)

    def rest_copy(slot, target, frame):
        return pltpu.make_async_remote_copy(rest_out.at[frame], rest_in.at[slot], rest_send_sem.at[slot], rest_recv_sem.at[slot], device_id={"occ": target}, device_id_type=MESH)

    hops = []
    for way, (d_chip, d_core) in enumerate(order[-CORES:]):
        frame = device(d_chip, d_core)
        leg = half // 2 if way == 0 else -(half // 2)
        via = device(leg, 0)
        hop = pltpu.make_async_remote_copy(local.at[frame, :, :, pl.ds(0, n_main)], relay.at[way], hop_send_sem.at[way], hop_recv_sem.at[way], device_id={"occ": via}, device_id_type=MESH)
        hop_rest = pltpu.make_async_remote_copy(rest_out.at[frame], relay_rest.at[way], hop_rest_send_sem.at[way], hop_rest_recv_sem.at[way], device_id={"occ": via}, device_id_type=MESH)
        slot = len(order) - CORES + way
        last = device(leg, d_core)
        onward = pltpu.make_async_remote_copy(relay.at[way], blocks.at[slot, :, :, pl.ds(0, n_main)], send_sem.at[slot], recv_sem.at[slot], device_id={"occ": last}, device_id_type=MESH)
        onward_rest = pltpu.make_async_remote_copy(relay_rest.at[way], rest_in.at[slot], rest_send_sem.at[slot], rest_recv_sem.at[slot], device_id={"occ": last}, device_id_type=MESH)
        hop.start()
        hop_rest.start()
        hops.append((hop, hop_rest, onward, onward_rest))
    for slot in range(1, len(order) - CORES):
        target = device(*order[slot])
        rest_copy(slot, target, target).start()
        main_copy(slot, target, target).start()

    own.wait()

    def energy(k_pair, eps_pair):
        terms = k_pair * (2.0 * k_pair - k_pair.T) / (eps_pair - vir_sum[...])
        return jnp.sum(terms.reshape(n_vir // 8, 8, n_vir), axis=0)

    def gram(rows, cols):
        return lax.dot_general(rows, cols, (((1,), (1,)), ((), ())), preferred_element_type=jnp.float32)

    def add_pair(slot_x, orb_x, slot_y, orb_y, k_pair):
        e_vec = energy(k_pair, eps_slot[slot_x, orb_x] + eps_slot[slot_y, orb_y]) * (act_slot[slot_x, orb_x] * act_slot[slot_y, orb_y])
        acc[slot_x, orb_x] += e_vec
        if not (slot_x is slot_y and orb_x == orb_y):
            acc[slot_y, orb_y] += e_vec

    def block_step(slot, carry):
        @pl.when(slot == 2)
        def _():
            for hop, hop_rest, onward, onward_rest in hops:
                hop.wait_recv()
                hop_rest.wait_recv()
                onward.start()
                onward_rest.start()

        @pl.when(slot > 0)
        def _():
            main_copy(slot, me, me).wait_recv()
            rest_copy(slot, me, me).wait_recv()
            tail = rest_in[slot]
            tail = jnp.concatenate([tail[:, part * n_rest:(part + 1) * n_rest] for part in range(fold)], axis=0)
            blocks[slot, :, :, n_main:] = tail.reshape(n_loc, n_vir, n_rest)

        mine = blocks[slot]
        for orb_x in range(n_loc):
            rows = mine[:orb_x + 1].reshape((orb_x + 1) * n_vir, n_aux)
            product = gram(rows, mine[orb_x])
            for orb_y in range(orb_x + 1):
                add_pair(slot, orb_x, slot, orb_y, product[orb_y * n_vir:(orb_y + 1) * n_vir])

        def with_earlier(prior, inner):
            rows = blocks[prior].reshape(n_loc * n_vir, n_aux)
            for orb_x in range(n_loc):
                product = gram(rows, blocks[slot, orb_x])
                for orb_y in range(n_loc):
                    add_pair(slot, orb_x, prior, orb_y, product[orb_y * n_vir:(orb_y + 1) * n_vir])
            return inner

        lax.fori_loop(0, slot, with_earlier, 0)
        return carry

    lax.fori_loop(0, n_dev, block_step, 0)

    e_orb = jnp.sum(jnp.sum(acc[...].reshape(n_dev * n_loc, 8, n_vir), axis=1), axis=1, keepdims=True)
    total = jnp.sum(e_orb, axis=0, keepdims=True)
    copies = []
    for slot, (d_chip, d_core) in enumerate(order):
        result[slot, 0:n_loc, :] = jnp.broadcast_to(e_orb[slot * n_loc:(slot + 1) * n_loc], (n_loc, LANES))
        result[slot, n_loc:n_loc + 1, :] = jnp.broadcast_to(total, (1, LANES))
    for slot in range(1, n_dev):
        main_copy(slot, me, me).wait_send()
        rest_copy(slot, me, me).wait_send()
    for hop, hop_rest, _, _ in hops:
        hop.wait_send()
        hop_rest.wait_send()
    keep = pltpu.make_async_copy(result.at[0], out_ref.at[me], own_sem)
    keep.start()
    for slot, (d_chip, d_core) in enumerate(order):
        if slot > 0:
            copies.append(pltpu.make_async_remote_copy(result.at[slot], out_ref.at[me], res_send_sem.at[slot], res_recv_sem.at[slot], device_id={"occ": device(-d_chip, d_core)}, device_id_type=MESH))
            copies[-1].start()
    keep.wait()
    for copy in copies:
        copy.wait()


def solution(mesh):
    n_dev = mesh.shape["occ"]

    def local_fn(b_own, eps_occ, eps_vir, active):
        b_rows = jnp.transpose(b_own, (0, 2, 3, 1))
        n_frame, n_loc, n_vir, n_aux = b_rows.shape
        n_main = n_aux // LANES * LANES
        fold = LANES // (n_aux - n_main)
        fold_rows = n_loc * n_vir // fold
        vmem, smem, sem = pltpu.VMEM, pltpu.SMEM, pltpu.SemaphoreType.DMA
        out = pl.pallas_call(
            functools.partial(kernel, n_dev),
            out_shape=jax.ShapeDtypeStruct((n_frame, 8, LANES), jnp.float32),
            in_specs=[pl.BlockSpec(memory_space=pl.ANY), pl.BlockSpec(memory_space=smem), pl.BlockSpec(memory_space=smem), pl.BlockSpec(memory_space=vmem)],
            out_specs=pl.BlockSpec(memory_space=vmem),
            scratch_shapes=[
                vmem(b_rows.shape, b_rows.dtype),
                vmem((n_dev, n_loc, n_vir, n_aux), b_rows.dtype),
                vmem((n_dev, fold_rows, LANES), b_rows.dtype),
                vmem((n_dev, fold_rows, LANES), b_rows.dtype),
                vmem((CORES, n_loc, n_vir, n_main), b_rows.dtype),
                vmem((CORES, fold_rows, LANES), b_rows.dtype),
                vmem((n_vir, n_vir), jnp.float32),
                vmem((n_dev, n_loc, 8, n_vir), jnp.float32),
                vmem((n_dev, 8, LANES), jnp.float32),
                smem((n_dev, n_loc), jnp.float32),
                smem((n_dev, n_loc), jnp.float32),
                sem, sem,
                sem((n_dev,)), sem((n_dev,)), sem((n_dev,)), sem((n_dev,)),
                sem((CORES,)), sem((CORES,)), sem((CORES,)), sem((CORES,)),
                sem((n_dev,)), sem((n_dev,)),
            ],
            compiler_params=pltpu.CompilerParams(collective_id=0, has_side_effects=True, vmem_limit_bytes=56 * 2**20),
            cost_estimate=pl.CostEstimate(flops=2 * n_vir * n_vir * n_aux * n_dev * n_loc * (n_dev * n_loc + 1) // 2, bytes_accessed=2 * b_rows.size * 2, transcendentals=0),
            name="pair_energies",
        )(b_rows, eps_occ, active, eps_vir)
        return out[:, 0:n_loc, 0], out[:, n_loc, 0]

    return jax.shard_map(local_fn, mesh=mesh, in_specs=(P("mol", None, "occ", None), P("mol", None), P("mol", None), P("mol", None)), out_specs=(P("mol", "occ"), P("mol")), check_vma=False)
```

```python
import functools

import jax
import jax.numpy as jnp
from jax import lax
from jax.experimental import pallas as pl
from jax.experimental.pallas import tpu as pltpu
from jax.sharding import PartitionSpec as P

MESH = pl.DeviceIdType.MESH
CORES = 2
LANES = 128


def schedule(n_chip, n_loc):
    half = n_chip // 2
    pairs = [[(dist, core), (-dist, core)] for dist in range(1, half) for core in range(CORES)]
    pairs.insert(0, [(half, core) for core in range(CORES)])
    sources = [(0, 0), (0, 1)] + [disp for pair in pairs for disp in pair]
    slots = [[(source, orb) for orb in range(n_loc)] for source in range(CORES)]
    for first in range(CORES, len(sources), n_loc):
        slots += [[(first + k, orb) for k in range(n_loc)] for orb in range(n_loc)]
    return sources, slots


def kernel(n_dev, b_hbm, eps_ref, act_ref, vir_ref, e_ref, total_ref, local, blocks, rest_out, rest_in, vir_sum, product, acc, result, returned, eps_slot, act_slot, load_sem, own_sem, send_sem, recv_sem, rest_send_sem, rest_recv_sem, res_send_sem, res_recv_sem):
    n_chip = n_dev // CORES
    n_slot, n_loc, n_vir, n_aux = blocks.shape
    sources, slots = schedule(n_chip, n_loc)
    n_main = n_aux // LANES * LANES
    n_rest = n_aux - n_main
    fold = LANES // n_rest
    fold_rows = n_loc * n_vir // fold
    me = lax.axis_index("occ")
    chip, core = me // CORES, me % CORES
    main = pl.ds(0, n_main)

    def device(d_chip, d_core):
        return (chip + d_chip + n_chip) % n_chip * CORES + (core + d_core) % CORES

    targets = [device(d_chip, d_core) for d_chip, d_core in sources]
    owners = [device(-d_chip, d_core) for d_chip, d_core in sources]

    barrier = pltpu.get_barrier_semaphore()
    for step in range(1, n_dev):
        pl.semaphore_signal(barrier, inc=1, device_id={"occ": (me + step) % n_dev}, device_id_type=MESH)
    load = pltpu.make_async_copy(b_hbm, local, load_sem)
    load.start()
    own = pltpu.make_async_copy(b_hbm.at[me], blocks.at[0], own_sem)
    own.start()

    for slot, members in enumerate(slots):
        for k, (source, orb) in enumerate(members):
            eps_slot[slot, k] = eps_ref[me, owners[source] * n_loc + orb]
            act_slot[slot, k] = act_ref[me, owners[source] * n_loc + orb].astype(jnp.float32)
    vir_row = jnp.broadcast_to(vir_ref[pl.ds(me, 1), :], (n_vir, n_vir))
    vir_sum[...] = vir_row + vir_row.T
    acc[...] = jnp.zeros_like(acc)
    load.wait()

    def pack(frame, carry):
        tail = local[frame, :, :, n_main:].reshape(n_loc * n_vir, n_rest)
        rest_out[frame] = jnp.concatenate([tail[part * fold_rows:(part + 1) * fold_rows] for part in range(fold)], axis=1)
        return carry

    lax.fori_loop(0, n_dev, pack, 0)
    pl.semaphore_wait(barrier, n_dev - 1)

    def main_copy(slot, k, orb, target):
        return pltpu.make_async_remote_copy(b_hbm.at[target, orb, :, main], blocks.at[slot, k, :, main], send_sem.at[slot, k], recv_sem.at[slot, k], device_id={"occ": target}, device_id_type=MESH)

    def rest_copy(source, target):
        return pltpu.make_async_remote_copy(rest_out.at[target], rest_in.at[source], rest_send_sem.at[source], rest_recv_sem.at[source], device_id={"occ": target}, device_id_type=MESH)

    for slot, members in enumerate(slots):
        for k, (source, orb) in enumerate(members):
            if source > 0:
                if orb == 0:
                    rest_copy(source, targets[source]).start()
                main_copy(slot, k, orb, targets[source]).start()
    own.wait()

    def multiply(slot, prior):
        rows = blocks[prior].reshape(n_loc * n_vir, n_aux)
        for x in range(n_loc):
            product[x] = lax.dot_general(rows, blocks[slot, x], (((1,), (1,)), ((), ())), preferred_element_type=jnp.float32)

    def add_energies(slot, prior):
        cross = jnp.where(slot == prior, 0.0, 1.0)
        columns = [None] * n_loc
        for x in range(n_loc):
            row = None
            for y in range(n_loc):
                k_pair = product[x, y * n_vir:(y + 1) * n_vir]
                terms = k_pair * (2.0 * k_pair - k_pair.T) / ((eps_slot[slot, x] + eps_slot[prior, y]) - vir_sum[...])
                e_vec = jnp.sum(terms.reshape(n_vir // 8, 8, n_vir), axis=0) * (act_slot[slot, x] * act_slot[prior, y])
                row = e_vec if row is None else row + e_vec
                columns[y] = e_vec if columns[y] is None else columns[y] + e_vec
            acc[slot, x] += row
        for y in range(n_loc):
            acc[prior, y] += columns[y] * cross

    def arrive(slot):
        def unpack(slot, k, source, orb):
            part_rows = n_vir // fold_rows if n_vir >= fold_rows else 1
            tail = rest_in[source]
            parts = [tail[:, part * n_rest:(part + 1) * n_rest] for part in range(orb * part_rows, (orb + 1) * part_rows)]
            blocks[slot, k, :, n_main:] = jnp.concatenate(parts, axis=0)

        for index, members in enumerate(slots):
            if index > 0:
                @pl.when(slot == index)
                def _(index=index, members=members):
                    for k, (source, orb) in enumerate(members):
                        if orb == 0:
                            rest_copy(source, me).wait_recv()
                        main_copy(index, k, orb, me).wait_recv()
                        unpack(index, k, source, orb)

    def slot_step(slot, carry):
        arrive(slot)

        def prior_step(prior, last):
            add_energies(*last)
            multiply(slot, prior)
            return slot, prior

        return lax.fori_loop(0, slot + 1, prior_step, carry)

    multiply(0, 0)
    last = lax.fori_loop(1, n_slot, slot_step, (jnp.int32(0), jnp.int32(0)))
    add_energies(*last)

    e_orb = jnp.sum(jnp.sum(acc[...].reshape(n_slot * n_loc, 8, n_vir), axis=1), axis=1, keepdims=True)
    total = jnp.sum(e_orb, axis=0, keepdims=True)
    where_is = {member: slot * n_loc + k for slot, members in enumerate(slots) for k, member in enumerate(members)}
    lane = lax.broadcasted_iota(jnp.int32, (8, LANES), 1)
    for source in range(n_dev):
        tile = jnp.broadcast_to(total, (8, LANES))
        for orb in range(n_loc):
            at = where_is[source, orb]
            tile = jnp.where(lane == orb, jnp.broadcast_to(e_orb[at:at + 1], (8, LANES)), tile)
        result[source] = tile
    for slot, members in enumerate(slots):
        for k, (source, orb) in enumerate(members):
            if source > 0:
                main_copy(slot, k, orb, me).wait_send()
                if orb == 0:
                    rest_copy(source, me).wait_send()
    copies = []
    for source in range(1, n_dev):
        copies.append(pltpu.make_async_remote_copy(result.at[source], returned.at[me], res_send_sem.at[source], res_recv_sem.at[source], device_id={"occ": owners[source]}, device_id_type=MESH))
        copies[-1].start()
    returned[me] = result[0]
    for copy in copies:
        copy.wait()
    rows = returned[:, 0, :]
    e_ref[...] = rows[:, 0:n_loc]
    total_ref[...] = rows.T[n_loc:n_loc + 1, :]


def solution(mesh):
    n_dev = mesh.shape["occ"]

    def local_fn(b_own, eps_occ, eps_vir, active):
        b_rows = jnp.transpose(b_own, (0, 2, 3, 1))
        n_frame, n_loc, n_vir, n_aux = b_rows.shape
        fold = LANES // (n_aux % LANES)
        fold_rows = n_loc * n_vir // fold
        n_orb = n_dev * n_loc
        vmem, smem, sem = pltpu.VMEM, pltpu.SMEM, pltpu.SemaphoreType.DMA
        e_pair, energy = pl.pallas_call(
            functools.partial(kernel, n_dev),
            out_shape=(jax.ShapeDtypeStruct((n_frame, n_loc), jnp.float32), jax.ShapeDtypeStruct((1, n_frame), jnp.float32)),
            in_specs=[pl.BlockSpec(memory_space=pl.ANY), pl.BlockSpec(memory_space=smem), pl.BlockSpec(memory_space=smem), pl.BlockSpec(memory_space=vmem)],
            out_specs=(pl.BlockSpec(memory_space=vmem), pl.BlockSpec(memory_space=vmem)),
            scratch_shapes=[
                vmem(b_rows.shape, b_rows.dtype),
                vmem((n_dev, n_loc, n_vir, n_aux), b_rows.dtype),
                vmem((n_dev, fold_rows, LANES), b_rows.dtype),
                vmem((n_dev, fold_rows, LANES), b_rows.dtype),
                vmem((n_vir, n_vir), jnp.float32),
                vmem((n_loc, n_loc * n_vir, n_vir), jnp.float32),
                vmem((n_dev, n_loc, 8, n_vir), jnp.float32),
                vmem((n_dev, 8, LANES), jnp.float32),
                vmem((n_dev, 8, LANES), jnp.float32),
                smem((n_dev, n_loc), jnp.float32),
                smem((n_dev, n_loc), jnp.float32),
                sem, sem,
                sem((n_dev, n_loc)), sem((n_dev, n_loc)), sem((n_dev,)), sem((n_dev,)),
                sem((n_dev,)), sem((n_dev,)),
            ],
            compiler_params=pltpu.CompilerParams(collective_id=0, has_side_effects=True, vmem_limit_bytes=56 * 2**20),
            cost_estimate=pl.CostEstimate(flops=n_vir * n_vir * n_aux * n_orb * (n_orb + 1), bytes_accessed=2 * b_rows.size * 2, transcendentals=0),
            name="pair_energies",
        )(b_rows, eps_occ, active, eps_vir)
        return e_pair, energy[0]

    return jax.shard_map(local_fn, mesh=mesh, in_specs=(P("mol", None, "occ", None), P("mol", None), P("mol", None), P("mol", None)), out_specs=(P("mol", "occ"), P("mol")), check_vma=False)
```

```python
import functools

import jax
import jax.numpy as jnp
from jax import lax
from jax.experimental import pallas as pl
from jax.experimental.pallas import tpu as pltpu
from jax.sharding import PartitionSpec as P

MESH = pl.DeviceIdType.MESH
CORES = 2
LANES = 128
GROUP = 4


def schedule(n_chip, n_loc):
    half = n_chip // 2
    pairs = [[(dist, core), (-dist, core)] for dist in range(1, half) for core in range(CORES)]
    pairs.insert(0, [(half, core) for core in range(CORES)])
    sources = [(0, 0), (0, 1)] + [disp for pair in pairs for disp in pair]
    slots = [[(source, orb) for orb in range(n_loc)] for source in range(CORES)]
    for first in range(CORES, len(sources), n_loc):
        slots += [[(first + k, orb) for k in range(n_loc)] for orb in range(n_loc)]
    return sources, slots


def kernel(n_dev, b_hbm, eps_hbm, act_hbm, vir_hbm, out_ref, eps_ref, act_ref, vir_ref, local, blocks, rest_out, rest_in, vir_sum, product, acc, result, returned, eps_slot, act_slot, small_sem, load_sem, own_sem, send_sem, recv_sem, rest_send_sem, rest_recv_sem, res_send_sem, res_recv_sem):
    n_chip = n_dev // CORES
    n_slot, n_loc, n_vir, n_aux = blocks.shape
    sources, slots = schedule(n_chip, n_loc)
    n_main = n_aux // LANES * LANES
    n_rest = n_aux - n_main
    fold = LANES // n_rest
    fold_rows = n_loc * n_vir // fold
    me = lax.axis_index("occ")
    chip, core = me // CORES, me % CORES
    main = pl.ds(0, n_main)

    def device(d_chip, d_core):
        return (chip + d_chip + n_chip) % n_chip * CORES + (core + d_core) % CORES

    targets = [device(d_chip, d_core) for d_chip, d_core in sources]
    owners = [device(-d_chip, d_core) for d_chip, d_core in sources]

    barrier = pltpu.get_barrier_semaphore()
    for step in range(1, n_dev):
        pl.semaphore_signal(barrier, inc=1, device_id={"occ": (me + step) % n_dev}, device_id_type=MESH)
    small = [pltpu.make_async_copy(source, target, small_sem.at[k]) for k, (source, target) in enumerate(((eps_hbm, eps_ref), (act_hbm, act_ref), (vir_hbm, vir_ref)))]
    for copy in small:
        copy.start()
    load = pltpu.make_async_copy(b_hbm, local, load_sem)
    load.start()
    own = pltpu.make_async_copy(b_hbm.at[me], blocks.at[0], own_sem)
    own.start()
    acc[...] = jnp.zeros_like(acc)
    for copy in small:
        copy.wait()

    for slot, members in enumerate(slots):
        for k, (source, orb) in enumerate(members):
            eps_slot[slot, k] = eps_ref[me, owners[source] * n_loc + orb]
            act_slot[slot, k] = act_ref[me, owners[source] * n_loc + orb].astype(jnp.float32)
    vir_row = jnp.broadcast_to(vir_ref[pl.ds(me, 1), :], (n_vir, n_vir))
    vir_sum[...] = vir_row + vir_row.T
    load.wait()

    def pack(frame, carry):
        tail = local[frame, :, :, n_main:].reshape(n_loc * n_vir, n_rest)
        rest_out[frame] = jnp.concatenate([tail[part * fold_rows:(part + 1) * fold_rows] for part in range(fold)], axis=1)
        return carry

    lax.fori_loop(0, n_dev, pack, 0)
    pl.semaphore_wait(barrier, n_dev - 1)

    def main_copy(slot, k, orb, target):
        return pltpu.make_async_remote_copy(b_hbm.at[target, orb, :, main], blocks.at[slot, k, :, main], send_sem.at[slot, k], recv_sem.at[slot, k], device_id={"occ": target}, device_id_type=MESH)

    def rest_copy(source, target):
        return pltpu.make_async_remote_copy(rest_out.at[target], rest_in.at[source], rest_send_sem.at[source], rest_recv_sem.at[source], device_id={"occ": target}, device_id_type=MESH)

    for slot, members in enumerate(slots):
        for k, (source, orb) in enumerate(members):
            if source > 0:
                if orb == 0:
                    rest_copy(source, targets[source]).start()
                main_copy(slot, k, orb, targets[source]).start()
    own.wait()

    def multiply(slot, first):
        rows = blocks[pl.ds(first, GROUP)].reshape(GROUP * n_loc * n_vir, n_aux)
        for x in range(n_loc):
            product[x] = lax.dot_general(rows, blocks[slot, x], (((1,), (1,)), ((), ())), preferred_element_type=jnp.float32)

    def fold_rows_of(terms):
        return jnp.sum(terms.reshape(terms.shape[0] // 8, 8, terms.shape[1]), axis=0)

    def pair_terms(k_ref, eps_pair):
        low, high = pl.ds(0, LANES), pl.ds(LANES, n_vir - LANES)
        def same(part):
            k_part = k_ref[part, part]
            return fold_rows_of(k_part * (2.0 * k_part - k_part.T) / (eps_pair - vir_sum[part, part]))
        k_ab, k_ba = k_ref[high, low], k_ref[low, high].T
        mixed = (2.0 * (k_ab * (k_ab - k_ba) + k_ba * k_ba)) / (eps_pair - vir_sum[high, low])
        return jnp.concatenate([same(low) + fold_rows_of(mixed), same(high)], axis=1)

    def add_energies(slot, first, fresh):
        row = [jnp.zeros(acc.shape[2:], jnp.float32)] * n_loc
        for g in range(GROUP):
            prior = first + g
            counts = jnp.where((prior >= fresh) & (prior <= slot), 1.0, 0.0)
            cross = jnp.where(prior == slot, 0.0, 1.0)
            for y in range(n_loc):
                column = None
                for x in range(n_loc):
                    at = (g * n_loc + y) * n_vir
                    e_vec = pair_terms(product.at[x, pl.ds(at, n_vir)], eps_slot[slot, x] + eps_slot[prior, y]) * (act_slot[slot, x] * act_slot[prior, y] * counts)
                    row[x] = row[x] + e_vec
                    column = e_vec if column is None else column + e_vec
                acc[prior, y] += column * cross
        for x in range(n_loc):
            acc[slot, x] += row[x]

    def arrive(slot, indices):
        def unpack(slot, k, source, orb):
            part_rows = n_vir // fold_rows if n_vir >= fold_rows else 1
            tail = rest_in[source]
            parts = [tail[:, part * n_rest:(part + 1) * n_rest] for part in range(orb * part_rows, (orb + 1) * part_rows)]
            blocks[slot, k, :, n_main:] = jnp.concatenate(parts, axis=0)

        for index in indices:
            @pl.when(slot == index)
            def _(index=index):
                for k, (source, orb) in enumerate(slots[index]):
                    if orb == 0:
                        rest_copy(source, me).wait_recv()
                    main_copy(index, k, orb, me).wait_recv()
                    unpack(index, k, source, orb)

    def slot_step(slot, carry):
        arrive(slot, range(GROUP, n_slot))

        def group_step(step, last):
            fresh = step * GROUP
            first = jnp.maximum(jnp.minimum(fresh, slot + 1 - GROUP), 0)
            add_energies(*last)
            multiply(slot, first)
            return slot, first, fresh

        return lax.fori_loop(0, slot // GROUP + 1, group_step, carry)

    for index in range(1, GROUP):
        arrive(index, [index])
    multiply(0, 0)
    last = lax.fori_loop(1, n_slot, slot_step, (jnp.int32(0), jnp.int32(0), jnp.int32(0)))
    add_energies(*last)

    e_orb = jnp.sum(jnp.sum(acc[...].reshape(n_slot * n_loc, 8, n_vir), axis=1), axis=1, keepdims=True)
    total = jnp.sum(e_orb, axis=0, keepdims=True)
    where_is = {member: slot * n_loc + k for slot, members in enumerate(slots) for k, member in enumerate(members)}
    lane = lax.broadcasted_iota(jnp.int32, (8, LANES), 1)
    for source in range(n_dev):
        tile = jnp.broadcast_to(total, (8, LANES))
        for orb in range(n_loc):
            at = where_is[source, orb]
            tile = jnp.where(lane == orb, jnp.broadcast_to(e_orb[at:at + 1], (8, LANES)), tile)
        result[source] = tile
    for slot, members in enumerate(slots):
        for k, (source, orb) in enumerate(members):
            if source > 0:
                main_copy(slot, k, orb, me).wait_send()
                if orb == 0:
                    rest_copy(source, me).wait_send()
    copies = []
    for source in range(1, n_dev):
        copies.append(pltpu.make_async_remote_copy(result.at[source, pl.ds(0, 1)], returned.at[me, pl.ds(0, 1)], res_send_sem.at[source], res_recv_sem.at[source], device_id={"occ": owners[source]}, device_id_type=MESH))
        copies[-1].start()
    returned[me] = result[0]
    for copy in copies:
        copy.wait()
    out_ref[...] = returned[:, 0, :].T[0:8]


def finish(rows_ref, e_ref, total_ref):
    e_ref[...] = rows_ref[0:e_ref.shape[0], :]
    total_ref[...] = rows_ref[e_ref.shape[0]:e_ref.shape[0] + 1, :]


def solution(mesh):
    n_dev = mesh.shape["occ"]

    def local_fn(b_own, eps_occ, eps_vir, active):
        b_rows = jnp.transpose(b_own, (0, 2, 3, 1))
        n_frame, n_loc, n_vir, n_aux = b_rows.shape
        fold = LANES // (n_aux % LANES)
        fold_rows = n_loc * n_vir // fold
        n_orb = n_dev * n_loc
        vmem, smem, sem = pltpu.VMEM, pltpu.SMEM, pltpu.SemaphoreType.DMA
        rows = pl.pallas_call(
            functools.partial(kernel, n_dev),
            out_shape=jax.ShapeDtypeStruct((8, n_frame), jnp.float32),
            in_specs=[pl.BlockSpec(memory_space=pl.ANY)] * 4,
            out_specs=pl.BlockSpec(memory_space=vmem),
            scratch_shapes=[
                smem(eps_occ.shape, eps_occ.dtype),
                smem(active.shape, active.dtype),
                vmem(eps_vir.shape, eps_vir.dtype),
                vmem(b_rows.shape, b_rows.dtype),
                vmem((n_dev, n_loc, n_vir, n_aux), b_rows.dtype),
                vmem((n_dev, fold_rows, LANES), b_rows.dtype),
                vmem((n_dev, fold_rows, LANES), b_rows.dtype),
                vmem((n_vir, n_vir), jnp.float32),
                vmem((n_loc, GROUP * n_loc * n_vir, n_vir), jnp.float32),
                vmem((n_dev, n_loc, 8, n_vir), jnp.float32),
                vmem((n_dev, 8, LANES), jnp.float32),
                vmem((n_dev, 8, LANES), jnp.float32),
                smem((n_dev, n_loc), jnp.float32),
                smem((n_dev, n_loc), jnp.float32),
                sem((3,)), sem, sem,
                sem((n_dev, n_loc)), sem((n_dev, n_loc)), sem((n_dev,)), sem((n_dev,)),
                sem((n_dev,)), sem((n_dev,)),
            ],
            compiler_params=pltpu.CompilerParams(collective_id=0, has_side_effects=True, vmem_limit_bytes=56 * 2**20),
            cost_estimate=pl.CostEstimate(flops=n_vir * n_vir * n_aux * n_orb * (n_orb + 1), bytes_accessed=2 * b_rows.size * 2, transcendentals=0),
            name="pair_energies",
        )(b_rows, eps_occ, active, eps_vir)
        e_pair, energy = pl.pallas_call(
            finish,
            out_shape=(jax.ShapeDtypeStruct((n_loc, n_frame), jnp.float32), jax.ShapeDtypeStruct((1, n_frame), jnp.float32)),
            in_specs=[pl.BlockSpec(memory_space=vmem)],
            out_specs=(pl.BlockSpec(memory_space=vmem), pl.BlockSpec(memory_space=vmem)),
            name="finish",
        )(rows)
        return e_pair.T, energy[0]

    return jax.shard_map(local_fn, mesh=mesh, in_specs=(P("mol", None, "occ", None), P("mol", None), P("mol", None), P("mol", None)), out_specs=(P("mol", "occ"), P("mol")), check_vma=False)
```

```python
import functools

import jax
import jax.numpy as jnp
from jax import lax
from jax.experimental import pallas as pl
from jax.experimental.pallas import tpu as pltpu
from jax.sharding import PartitionSpec as P

MESH = pl.DeviceIdType.MESH
CORES = 2
LANES = 128
SPLIT = 256
GROUP = 4


def schedule(n_chip, n_loc):
    half = n_chip // 2
    pairs = [[(dist, core), (-dist, core)] for dist in range(1, half) for core in range(CORES)]
    pairs.insert(0, [(half, core) for core in range(CORES)])
    sources = [(0, 0), (0, 1)] + [disp for pair in pairs for disp in pair]
    slots = [[(source, orb) for orb in range(n_loc)] for source in range(CORES)]
    for first in range(CORES, len(sources), n_loc):
        slots += [[(first + k, orb) for k in range(n_loc)] for orb in range(n_loc)]
    return sources, slots


def kernel(n_dev, b_hbm, eps_hbm, act_hbm, vir_hbm, out_ref, eps_ref, act_ref, vir_ref, local, blocks, rest_out, rest_in, vir_sum, product, partial, acc, result, returned, eps_slot, act_slot, small_sem, load_sem, own_sem, send_sem, recv_sem, late_send_sem, late_recv_sem, rest_send_sem, rest_recv_sem, res_send_sem, res_recv_sem):
    n_chip = n_dev // CORES
    n_slot, n_loc, n_vir, n_aux = blocks.shape
    sources, slots = schedule(n_chip, n_loc)
    n_main = n_aux // LANES * LANES
    n_rest = n_aux - n_main
    fold = LANES // n_rest
    fold_rows = n_loc * n_vir // fold
    me = lax.axis_index("occ")
    chip, core = me // CORES, me % CORES
    main, head = pl.ds(0, n_main), pl.ds(0, SPLIT)

    def device(d_chip, d_core):
        return (chip + d_chip + n_chip) % n_chip * CORES + (core + d_core) % CORES

    targets = [device(d_chip, d_core) for d_chip, d_core in sources]
    owners = [device(-d_chip, d_core) for d_chip, d_core in sources]

    barrier = pltpu.get_barrier_semaphore()
    for step in range(1, n_dev):
        pl.semaphore_signal(barrier, inc=1, device_id={"occ": (me + step) % n_dev}, device_id_type=MESH)
    load = pltpu.make_async_copy(b_hbm.at[:, :, :, pl.ds(n_main, n_rest)], local, load_sem)
    load.start()
    own = pltpu.make_async_copy(b_hbm.at[me], blocks.at[0], own_sem)
    own.start()
    small = [pltpu.make_async_copy(source, target, small_sem.at[k]) for k, (source, target) in enumerate(((eps_hbm, eps_ref), (act_hbm, act_ref), (vir_hbm, vir_ref)))]
    for copy in small:
        copy.start()

    def lanes_copy(slot, k, orb, target, lanes, sends, recvs):
        return pltpu.make_async_remote_copy(b_hbm.at[target, orb, :, lanes], blocks.at[slot, k, :, lanes], sends, recvs, device_id={"occ": target}, device_id_type=MESH)

    def main_copy(slot, k, orb, target):
        lanes = head if slot == n_slot - 1 else main
        return lanes_copy(slot, k, orb, target, lanes, send_sem.at[slot, k], recv_sem.at[slot, k])

    def late_copy(k, orb, target):
        return lanes_copy(n_slot - 1, k, orb, target, pl.ds(SPLIT, n_main - SPLIT), late_send_sem.at[k], late_recv_sem.at[k])

    def rest_copy(source, target):
        return pltpu.make_async_remote_copy(rest_out.at[target], rest_in.at[source], rest_send_sem.at[source], rest_recv_sem.at[source], device_id={"occ": target}, device_id_type=MESH)

    def send_slots(indices):
        for slot in indices:
            for k, (source, orb) in enumerate(slots[slot]):
                main_copy(slot, k, orb, targets[source]).start()

    def pack(frame, carry):
        tail = local[frame].reshape(n_loc * n_vir, n_rest)
        rest_out[frame] = jnp.concatenate([tail[part * fold_rows:(part + 1) * fold_rows] for part in range(fold)], axis=1)
        return carry

    load.wait()
    lax.fori_loop(0, n_dev, pack, 0)
    pl.semaphore_wait(barrier, n_dev - 1)
    for source in range(1, n_dev):
        rest_copy(source, targets[source]).start()
    send_slots(range(1, n_slot))
    for k, (source, orb) in enumerate(slots[-1]):
        late_copy(k, orb, targets[source]).start()

    acc[...] = jnp.zeros_like(acc)
    result[...] = jnp.zeros_like(result)
    for copy in small:
        copy.wait()
    for slot, members in enumerate(slots):
        for k, (source, orb) in enumerate(members):
            eps_slot[slot, k] = eps_ref[me, owners[source] * n_loc + orb]
            act_slot[slot, k] = act_ref[me, owners[source] * n_loc + orb].astype(jnp.float32)
    vir_row = jnp.broadcast_to(vir_ref[pl.ds(me, 1), :], (n_vir, n_vir))
    vir_sum[...] = vir_row + vir_row.T
    own.wait()

    def gram(slot, x, first, lanes):
        rows = blocks[pl.ds(first, GROUP), :, :, lanes]
        cols = blocks[slot, x, :, lanes]
        return lax.dot_general(rows.reshape(GROUP * n_loc * n_vir, cols.shape[1]), cols, (((1,), (1,)), ((), ())), preferred_element_type=jnp.float32)

    def multiply(slot, first):
        for x in range(n_loc):
            product[x] = gram(slot, x, first, slice(None))

    def fold_rows_of(terms):
        return jnp.sum(terms.reshape(terms.shape[0] // 8, 8, terms.shape[1]), axis=0)

    def pair_terms(k_ref, eps_pair):
        low, high = pl.ds(0, LANES), pl.ds(LANES, n_vir - LANES)
        def same(part):
            k_part = k_ref[part, part]
            return fold_rows_of(k_part * (2.0 * k_part - k_part.T) / (eps_pair - vir_sum[part, part]))
        k_ab, k_ba = k_ref[high, low], k_ref[low, high].T
        mixed = (2.0 * (k_ab * (k_ab - k_ba) + k_ba * k_ba)) / (eps_pair - vir_sum[high, low])
        return jnp.concatenate([same(low) + fold_rows_of(mixed), same(high)], axis=1)

    def add_energies(slot, first, fresh):
        row = [jnp.zeros(acc.shape[2:], jnp.float32)] * n_loc
        for g in range(GROUP):
            prior = first + g
            counts = jnp.where((prior >= fresh) & (prior <= slot), 1.0, 0.0)
            cross = jnp.where(prior == slot, 0.0, 1.0)
            for y in range(n_loc):
                column = None
                for x in range(n_loc):
                    at = (g * n_loc + y) * n_vir
                    e_vec = pair_terms(product.at[x, pl.ds(at, n_vir)], eps_slot[slot, x] + eps_slot[prior, y]) * (act_slot[slot, x] * act_slot[prior, y] * counts)
                    row[x] = row[x] + e_vec
                    column = e_vec if column is None else column + e_vec
                acc[prior, y] += column * cross
        for x in range(n_loc):
            acc[slot, x] += row[x]

    def unpack(slot, k, source, orb):
        part_rows = n_vir // fold_rows if n_vir >= fold_rows else 1
        tail = rest_in[source]
        parts = [tail[:, part * n_rest:(part + 1) * n_rest] for part in range(orb * part_rows, (orb + 1) * part_rows)]
        blocks[slot, k, :, n_main:] = jnp.concatenate(parts, axis=0)

    def arrive(slot, indices):
        for index in indices:
            @pl.when(slot == index)
            def _(index=index):
                for k, (source, orb) in enumerate(slots[index]):
                    if orb == 0:
                        rest_copy(source, me).wait_recv()
                    main_copy(index, k, orb, me).wait_recv()
                    unpack(index, k, source, orb)

    def slot_step(slot, carry):
        arrive(slot, range(GROUP, n_slot - 1))

        def group_step(step, last):
            fresh = step * GROUP
            first = jnp.maximum(jnp.minimum(fresh, slot + 1 - GROUP), 0)
            add_energies(*last)
            multiply(slot, first)
            return slot, first, fresh

        return lax.fori_loop(0, slot // GROUP + 1, group_step, carry)

    for index in range(1, GROUP):
        arrive(index, [index])
    multiply(0, 0)
    last = lax.fori_loop(1, n_slot - 1, slot_step, (jnp.int32(0), jnp.int32(0), jnp.int32(0)))
    add_energies(*last)

    final = n_slot - 1
    for k, (source, orb) in enumerate(slots[final]):
        main_copy(final, k, orb, me).wait_recv()

    def head_step(step, carry):
        for x in range(n_loc):
            partial[step, x] = gram(final, x, step * GROUP, slice(0, SPLIT))
        return carry

    lax.fori_loop(0, n_slot // GROUP, head_step, 0)
    for k, (source, orb) in enumerate(slots[final]):
        late_copy(k, orb, me).wait_recv()
        unpack(final, k, source, orb)

    def finish_product(step):
        for x in range(n_loc):
            product[x] = partial[step, x] + gram(final, x, step * GROUP, slice(SPLIT, n_aux))

    def tail_step(step, carry):
        add_energies(final, (step - 1) * GROUP, (step - 1) * GROUP)
        finish_product(step)
        return carry

    finish_product(0)
    lax.fori_loop(1, n_slot // GROUP, tail_step, 0)
    add_energies(final, n_slot - GROUP, n_slot - GROUP)

    e_orb = jnp.sum(jnp.sum(acc[...].reshape(n_slot * n_loc, 8, n_vir), axis=1), axis=1, keepdims=True)
    total = jnp.sum(e_orb, axis=0, keepdims=True)
    where_is = {member: slot * n_loc + k for slot, members in enumerate(slots) for k, member in enumerate(members)}
    lane = lax.broadcasted_iota(jnp.int32, (8, LANES), 1)
    for source in range(n_dev):
        tile = jnp.broadcast_to(total, (8, LANES))
        for orb in range(n_loc):
            at = where_is[source, orb]
            tile = jnp.where(lane == orb, jnp.broadcast_to(e_orb[at:at + 1], (8, LANES)), tile)
        result[source] = tile
    for slot, members in enumerate(slots):
        for k, (source, orb) in enumerate(members):
            if source > 0:
                main_copy(slot, k, orb, me).wait_send()
                if slot == final:
                    late_copy(k, orb, me).wait_send()
                if orb == 0:
                    rest_copy(source, me).wait_send()
    copies = []
    for source in range(1, n_dev):
        copies.append(pltpu.make_async_remote_copy(result.at[source, pl.ds(0, 1)], returned.at[me, pl.ds(0, 1)], res_send_sem.at[source], res_recv_sem.at[source], device_id={"occ": owners[source]}, device_id_type=MESH))
        copies[-1].start()
    returned[me] = result[0]
    for copy in copies:
        copy.wait()
    out_ref[...] = returned[:, 0, :].T[0:8]


def finish(rows_ref, e_ref, total_ref):
    e_ref[...] = rows_ref[0:e_ref.shape[0], :]
    total_ref[...] = rows_ref[e_ref.shape[0]:e_ref.shape[0] + 1, :]


def solution(mesh):
    n_dev = mesh.shape["occ"]

    def local_fn(b_own, eps_occ, eps_vir, active):
        b_rows = jnp.transpose(b_own, (0, 2, 3, 1))
        n_frame, n_loc, n_vir, n_aux = b_rows.shape
        fold = LANES // (n_aux % LANES)
        fold_rows = n_loc * n_vir // fold
        n_orb = n_dev * n_loc
        vmem, smem, sem = pltpu.VMEM, pltpu.SMEM, pltpu.SemaphoreType.DMA
        rows = pl.pallas_call(
            functools.partial(kernel, n_dev),
            out_shape=jax.ShapeDtypeStruct((8, n_frame), jnp.float32),
            in_specs=[pl.BlockSpec(memory_space=pl.ANY)] * 4,
            out_specs=pl.BlockSpec(memory_space=vmem),
            scratch_shapes=[
                smem(eps_occ.shape, eps_occ.dtype),
                smem(active.shape, active.dtype),
                vmem(eps_vir.shape, eps_vir.dtype),
                vmem((n_frame, n_loc, n_vir, n_aux % LANES), b_rows.dtype),
                vmem((n_dev, n_loc, n_vir, n_aux), b_rows.dtype),
                vmem((n_dev, fold_rows, LANES), b_rows.dtype),
                vmem((n_dev, fold_rows, LANES), b_rows.dtype),
                vmem((n_vir, n_vir), jnp.float32),
                vmem((n_loc, GROUP * n_loc * n_vir, n_vir), jnp.float32),
                vmem((n_dev // GROUP, n_loc, GROUP * n_loc * n_vir, n_vir), jnp.float32),
                vmem((n_dev, n_loc, 8, n_vir), jnp.float32),
                vmem((n_dev, 8, LANES), jnp.float32),
                vmem((n_dev, 8, LANES), jnp.float32),
                smem((n_dev, n_loc), jnp.float32),
                smem((n_dev, n_loc), jnp.float32),
                sem((3,)), sem, sem,
                sem((n_dev, n_loc)), sem((n_dev, n_loc)), sem((n_loc,)), sem((n_loc,)), sem((n_dev,)), sem((n_dev,)),
                sem((n_dev,)), sem((n_dev,)),
            ],
            compiler_params=pltpu.CompilerParams(collective_id=0, has_side_effects=True, vmem_limit_bytes=56 * 2**20),
            cost_estimate=pl.CostEstimate(flops=n_vir * n_vir * n_aux * n_orb * (n_orb + 1), bytes_accessed=2 * b_rows.size * 2, transcendentals=0),
            name="pair_energies",
        )(b_rows, eps_occ, active, eps_vir)
        e_pair, energy = pl.pallas_call(
            finish,
            out_shape=(jax.ShapeDtypeStruct((n_loc, n_frame), jnp.float32), jax.ShapeDtypeStruct((1, n_frame), jnp.float32)),
            in_specs=[pl.BlockSpec(memory_space=vmem)],
            out_specs=(pl.BlockSpec(memory_space=vmem), pl.BlockSpec(memory_space=vmem)),
            name="finish",
        )(rows)
        return e_pair.T, energy[0]

    return jax.shard_map(local_fn, mesh=mesh, in_specs=(P("mol", None, "occ", None), P("mol", None), P("mol", None), P("mol", None)), out_specs=(P("mol", "occ"), P("mol")), check_vma=False)
```

```python
import functools

import jax
import jax.numpy as jnp
from jax import lax
from jax.experimental import pallas as pl
from jax.experimental.pallas import tpu as pltpu
from jax.sharding import PartitionSpec as P

MESH = pl.DeviceIdType.MESH
CORES = 2
LANES = 128
SPLIT = 256
GROUP = 4


def schedule(n_chip, n_loc):
    half = n_chip // 2
    pairs = [[(dist, core), (-dist, core)] for dist in range(1, half) for core in range(CORES)]
    pairs.insert(0, [(half, core) for core in range(CORES)])
    sources = [(0, 0), (0, 1)] + [disp for pair in pairs for disp in pair]
    slots = [[(source, orb) for orb in range(n_loc)] for source in range(CORES)]
    for first in range(CORES, len(sources), n_loc):
        slots += [[(first + k, orb) for k in range(n_loc)] for orb in range(n_loc)]
    return sources, slots


def kernel(n_dev, b_hbm, eps_hbm, act_hbm, vir_hbm, out_ref, eps_ref, act_ref, vir_ref, local, blocks, rest_out, rest_in, vir_sum, product, partial, acc, result, returned, eps_slot, act_slot, small_sem, load_sem, own_sem, send_sem, recv_sem, late_send_sem, late_recv_sem, rest_send_sem, rest_recv_sem, res_send_sem, res_recv_sem):
    n_chip = n_dev // CORES
    n_slot, n_loc, n_vir, n_aux = blocks.shape
    sources, slots = schedule(n_chip, n_loc)
    n_main = n_aux // LANES * LANES
    n_rest = n_aux - n_main
    fold = LANES // n_rest
    fold_rows = n_loc * n_vir // fold
    me = lax.axis_index("occ")
    chip, core = me // CORES, me % CORES
    main, head = pl.ds(0, n_main), pl.ds(0, SPLIT)

    def device(d_chip, d_core):
        return (chip + d_chip + n_chip) % n_chip * CORES + (core + d_core) % CORES

    targets = [device(d_chip, d_core) for d_chip, d_core in sources]
    owners = [device(-d_chip, d_core) for d_chip, d_core in sources]

    barrier = pltpu.get_barrier_semaphore()
    for step in range(1, n_dev):
        pl.semaphore_signal(barrier, inc=1, device_id={"occ": (me + step) % n_dev}, device_id_type=MESH)
    load = pltpu.make_async_copy(b_hbm.at[:, :, :, pl.ds(n_main, n_rest)], local, load_sem)
    load.start()
    own = pltpu.make_async_copy(b_hbm.at[me], blocks.at[0], own_sem)
    own.start()
    small = [pltpu.make_async_copy(source, target, small_sem.at[k]) for k, (source, target) in enumerate(((eps_hbm, eps_ref), (act_hbm, act_ref), (vir_hbm, vir_ref)))]
    for copy in small:
        copy.start()

    def lanes_copy(slot, k, orb, target, lanes, sends, recvs):
        return pltpu.make_async_remote_copy(b_hbm.at[target, orb, :, lanes], blocks.at[slot, k, :, lanes], sends, recvs, device_id={"occ": target}, device_id_type=MESH)

    def main_copy(slot, k, orb, target):
        lanes = head if slot == n_slot - 1 else main
        return lanes_copy(slot, k, orb, target, lanes, send_sem.at[slot, k], recv_sem.at[slot, k])

    def late_copy(k, orb, target):
        return lanes_copy(n_slot - 1, k, orb, target, pl.ds(SPLIT, n_main - SPLIT), late_send_sem.at[k], late_recv_sem.at[k])

    def rest_copy(source, target):
        return pltpu.make_async_remote_copy(rest_out.at[target], rest_in.at[source], rest_send_sem.at[source], rest_recv_sem.at[source], device_id={"occ": target}, device_id_type=MESH)

    def send_slots(indices):
        for slot in indices:
            for k, (source, orb) in enumerate(slots[slot]):
                main_copy(slot, k, orb, targets[source]).start()

    def pack(frame, carry):
        tail = local[frame].reshape(n_loc * n_vir, n_rest)
        rest_out[frame] = jnp.concatenate([tail[part * fold_rows:(part + 1) * fold_rows] for part in range(fold)], axis=1)
        return carry

    load.wait()
    lax.fori_loop(0, n_dev, pack, 0)
    pl.semaphore_wait(barrier, n_dev - 1)
    for source in range(1, n_dev):
        rest_copy(source, targets[source]).start()
    send_slots(range(1, n_slot))
    for k, (source, orb) in enumerate(slots[-1]):
        late_copy(k, orb, targets[source]).start()

    acc[...] = jnp.zeros_like(acc)
    result[...] = jnp.zeros_like(result)
    for copy in small:
        copy.wait()
    for slot, members in enumerate(slots):
        for k, (source, orb) in enumerate(members):
            eps_slot[slot, k] = eps_ref[me, owners[source] * n_loc + orb]
            act_slot[slot, k] = act_ref[me, owners[source] * n_loc + orb].astype(jnp.float32)
    vir_row = jnp.broadcast_to(vir_ref[pl.ds(me, 1), :], (n_vir, n_vir))
    vir_sum[...] = vir_row + vir_row.T
    own.wait()

    def gram(slot, x, first, lanes):
        rows = blocks[pl.ds(first, GROUP), :, :, lanes]
        cols = blocks[slot, x, :, lanes]
        return lax.dot_general(rows.reshape(GROUP * n_loc * n_vir, cols.shape[1]), cols, (((1,), (1,)), ((), ())), preferred_element_type=jnp.float32)

    def multiply(slot, first):
        for x in range(n_loc):
            product[x] = gram(slot, x, first, slice(None))

    def fold_rows_of(terms):
        return jnp.sum(terms.reshape(terms.shape[0] // 8, 8, terms.shape[1]), axis=0)

    def pair_terms(k_ref, eps_pair):
        low, high = pl.ds(0, LANES), pl.ds(LANES, n_vir - LANES)
        def same(part):
            k_part = k_ref[part, part]
            return fold_rows_of(k_part * (2.0 * k_part - k_part.T) / (eps_pair - vir_sum[part, part]))
        k_ab, k_ba = k_ref[high, low], k_ref[low, high].T
        mixed = (k_ab * (k_ab - k_ba) + k_ba * k_ba) / (eps_pair - vir_sum[high, low])
        return jnp.concatenate([same(low) + 2.0 * fold_rows_of(mixed), same(high)], axis=1)

    def add_energies(slot, first, fresh):
        row = [jnp.zeros(acc.shape[2:], jnp.float32)] * n_loc
        for g in range(GROUP):
            prior = first + g
            counts = jnp.where((prior >= fresh) & (prior <= slot), 1.0, 0.0)
            cross = jnp.where(prior == slot, 0.0, 1.0)
            for y in range(n_loc):
                column = None
                for x in range(n_loc):
                    at = (g * n_loc + y) * n_vir
                    e_vec = pair_terms(product.at[x, pl.ds(at, n_vir)], eps_slot[slot, x] + eps_slot[prior, y]) * (act_slot[slot, x] * act_slot[prior, y] * counts)
                    row[x] = row[x] + e_vec
                    column = e_vec if column is None else column + e_vec
                acc[prior, y] += column * cross
        for x in range(n_loc):
            acc[slot, x] += row[x]

    def unpack(slot, k, source, orb):
        part_rows = n_vir // fold_rows if n_vir >= fold_rows else 1
        tail = rest_in[source]
        parts = [tail[:, part * n_rest:(part + 1) * n_rest] for part in range(orb * part_rows, (orb + 1) * part_rows)]
        blocks[slot, k, :, n_main:] = jnp.concatenate(parts, axis=0)

    def arrive(slot, indices):
        for index in indices:
            @pl.when(slot == index)
            def _(index=index):
                for k, (source, orb) in enumerate(slots[index]):
                    if orb == 0:
                        rest_copy(source, me).wait_recv()
                    main_copy(index, k, orb, me).wait_recv()
                    unpack(index, k, source, orb)

    def slot_step(slot, carry):
        arrive(slot, range(GROUP, n_slot - 1))

        def group_step(step, last):
            fresh = step * GROUP
            first = jnp.maximum(jnp.minimum(fresh, slot + 1 - GROUP), 0)
            add_energies(*last)
            multiply(slot, first)
            return slot, first, fresh

        return lax.fori_loop(0, slot // GROUP + 1, group_step, carry)

    for index in range(1, GROUP):
        arrive(index, [index])
    multiply(0, 0)
    last = lax.fori_loop(1, n_slot - 1, slot_step, (jnp.int32(0), jnp.int32(0), jnp.int32(0)))
    add_energies(*last)

    final = n_slot - 1
    for k, (source, orb) in enumerate(slots[final]):
        main_copy(final, k, orb, me).wait_recv()

    def head_step(step, carry):
        for x in range(n_loc):
            partial[step, x] = gram(final, x, step * GROUP, slice(0, SPLIT))
        return carry

    lax.fori_loop(0, n_slot // GROUP, head_step, 0)
    for k, (source, orb) in enumerate(slots[final]):
        late_copy(k, orb, me).wait_recv()
        unpack(final, k, source, orb)

    def finish_product(step):
        for x in range(n_loc):
            product[x] = partial[step, x] + gram(final, x, step * GROUP, slice(SPLIT, n_aux))

    def tail_step(step, carry):
        add_energies(final, (step - 1) * GROUP, (step - 1) * GROUP)
        finish_product(step)
        return carry

    finish_product(0)
    lax.fori_loop(1, n_slot // GROUP, tail_step, 0)
    add_energies(final, n_slot - GROUP, n_slot - GROUP)

    e_orb = jnp.sum(jnp.sum(acc[...].reshape(n_slot * n_loc, 8, n_vir), axis=1), axis=1, keepdims=True)
    total = jnp.sum(e_orb, axis=0, keepdims=True)
    where_is = {member: slot * n_loc + k for slot, members in enumerate(slots) for k, member in enumerate(members)}
    lane = lax.broadcasted_iota(jnp.int32, (8, LANES), 1)
    for source in range(n_dev):
        tile = jnp.broadcast_to(total, (8, LANES))
        for orb in range(n_loc):
            at = where_is[source, orb]
            tile = jnp.where(lane == orb, jnp.broadcast_to(e_orb[at:at + 1], (8, LANES)), tile)
        result[source] = tile
    for slot, members in enumerate(slots):
        for k, (source, orb) in enumerate(members):
            if source > 0:
                main_copy(slot, k, orb, me).wait_send()
                if slot == final:
                    late_copy(k, orb, me).wait_send()
                if orb == 0:
                    rest_copy(source, me).wait_send()
    copies = []
    for source in range(1, n_dev):
        copies.append(pltpu.make_async_remote_copy(result.at[source, pl.ds(0, 1)], returned.at[me, pl.ds(0, 1)], res_send_sem.at[source], res_recv_sem.at[source], device_id={"occ": owners[source]}, device_id_type=MESH))
        copies[-1].start()
    returned[me] = result[0]
    for copy in copies:
        copy.wait()
    out_ref[...] = returned[:, 0, :].T[0:8]


def finish(rows_ref, e_ref, total_ref):
    e_ref[...] = rows_ref[0:e_ref.shape[0], :]
    total_ref[...] = rows_ref[e_ref.shape[0]:e_ref.shape[0] + 1, :]


def solution(mesh):
    n_dev = mesh.shape["occ"]

    def local_fn(b_own, eps_occ, eps_vir, active):
        b_rows = jnp.transpose(b_own, (0, 2, 3, 1))
        n_frame, n_loc, n_vir, n_aux = b_rows.shape
        fold = LANES // (n_aux % LANES)
        fold_rows = n_loc * n_vir // fold
        n_orb = n_dev * n_loc
        vmem, smem, sem = pltpu.VMEM, pltpu.SMEM, pltpu.SemaphoreType.DMA
        rows = pl.pallas_call(
            functools.partial(kernel, n_dev),
            out_shape=jax.ShapeDtypeStruct((8, n_frame), jnp.float32),
            in_specs=[pl.BlockSpec(memory_space=pl.ANY)] * 4,
            out_specs=pl.BlockSpec(memory_space=vmem),
            scratch_shapes=[
                smem(eps_occ.shape, eps_occ.dtype),
                smem(active.shape, active.dtype),
                vmem(eps_vir.shape, eps_vir.dtype),
                vmem((n_frame, n_loc, n_vir, n_aux % LANES), b_rows.dtype),
                vmem((n_dev, n_loc, n_vir, n_aux), b_rows.dtype),
                vmem((n_dev, fold_rows, LANES), b_rows.dtype),
                vmem((n_dev, fold_rows, LANES), b_rows.dtype),
                vmem((n_vir, n_vir), jnp.float32),
                vmem((n_loc, GROUP * n_loc * n_vir, n_vir), jnp.float32),
                vmem((n_dev // GROUP, n_loc, GROUP * n_loc * n_vir, n_vir), jnp.float32),
                vmem((n_dev, n_loc, 8, n_vir), jnp.float32),
                vmem((n_dev, 8, LANES), jnp.float32),
                vmem((n_dev, 8, LANES), jnp.float32),
                smem((n_dev, n_loc), jnp.float32),
                smem((n_dev, n_loc), jnp.float32),
                sem((3,)), sem, sem,
                sem((n_dev, n_loc)), sem((n_dev, n_loc)), sem((n_loc,)), sem((n_loc,)), sem((n_dev,)), sem((n_dev,)),
                sem((n_dev,)), sem((n_dev,)),
            ],
            compiler_params=pltpu.CompilerParams(collective_id=0, has_side_effects=True, vmem_limit_bytes=56 * 2**20),
            cost_estimate=pl.CostEstimate(flops=n_vir * n_vir * n_aux * n_orb * (n_orb + 1), bytes_accessed=2 * b_rows.size * 2, transcendentals=0),
            name="pair_energies",
        )(b_rows, eps_occ, active, eps_vir)
        e_pair, energy = pl.pallas_call(
            finish,
            out_shape=(jax.ShapeDtypeStruct((n_loc, n_frame), jnp.float32), jax.ShapeDtypeStruct((1, n_frame), jnp.float32)),
            in_specs=[pl.BlockSpec(memory_space=vmem)],
            out_specs=(pl.BlockSpec(memory_space=vmem), pl.BlockSpec(memory_space=vmem)),
            name="finish",
        )(rows)
        return e_pair.T, energy[0]

    return jax.shard_map(local_fn, mesh=mesh, in_specs=(P("mol", None, "occ", None), P("mol", None), P("mol", None), P("mol", None)), out_specs=(P("mol", "occ"), P("mol")), check_vma=False)
```
